32 devices in a mesh: dp: 8 (over z, x), fsdp: 4 (over y, core).
Axes of the slice: x: 2, y: 2, z: 4, core: 2. Of those that a mesh axis runs over, the one named last changes fastest.
Arguments:
- patches: bfloat16 [8, 4, 192, 64], P('dp', 'fsdp'), may hold values from -6 to 6
- noise: bfloat16 [8, 4, 192, 64], P('dp', 'fsdp'), may hold values from -6 to 6
- bucket: int32 [8, 4], P(None, 'fsdp'), may hold values from 0 to 11
- tstep: int32 [8, 4], P('dp', 'fsdp'), may hold values from 0 to 999
- dest: int32 [8, 4], P(None, 'fsdp'), may hold values from 0 to 7, as said below
- embed_weight: bfloat16 [64, 2432], replicated, may hold values from -0.75 to 0.75
- gain: float32 [2432], replicated, may hold values from 0.1 to 1.9
- proj_weight: bfloat16 [2432, 1216], P('fsdp'), may hold values from -0.125 to 0.125
- cotangent: bfloat16 [8, 4, 2, 192, 1216], P('dp', 'fsdp'), may hold values from -6 to 6
Outputs:
- projected: bfloat16 [8, 4, 2, 192, 1216], P('dp', 'fsdp')
- embed_grad: float32 [64, 2432], replicated
The draws below stay inside these ranges and needn't reach their ends.
Inputs may be any that keep to these rules, and one draw needn't show every extreme that they name: `dest`: in every column f, each dp index is named by at most 2 images and by exactly 2 for some.
All inputs are finite; a program needn't handle non-finite values.
Results may differ from the reference program's by a relative error of at most 0.006.
Values may be sent and summed in bfloat16 or wider, within the bound.
A program may use at most 64 MiB of HBM per device.

```python
import jax
import jax.numpy as jnp
from jax import lax

D = 2432
PATCH = 64
TOK_MAX = 192
CAP = 2
BUCKETS = 12
TSTEPS = 1000
HW = 1216
N_DP = 8
N_FSDP = 4


def draw_dest(key, part):

    def column(col):
        sub = jax.random.fold_in(key, col)
        owners = jax.random.permutation(jax.random.fold_in(sub, 11), N_DP).astype(jnp.int32)
        paired = jax.random.randint(jax.random.fold_in(sub, 12), (N_DP // 2,), 0, 2)
        paired = paired.at[0].set(1)
        first = owners[0::2]
        second = owners[1::2]
        other = jnp.where(paired == 1, first, second)
        targets = jnp.concatenate([first, other])
        order = jax.random.permutation(jax.random.fold_in(sub, 13), N_DP)
        return targets[order].astype(jnp.int32)
    return jax.vmap(column, out_axes=1)(jnp.arange(N_FSDP))


def touch_ends(entries, key, smallest, largest):
    dims = entries.shape
    place = [jax.random.randint(jax.random.fold_in(key, axis), (), 0, dims[axis]) for axis in range(len(dims))]
    entries = entries.at[tuple(place)].set(smallest)
    longest = dims.index(max(dims))
    place[longest] = (place[longest] + 1) % dims[longest]
    return entries.at[tuple(place)].set(largest)


def levels(stream_key, extent, pieces, low, high):
    level = 1.0
    for dim, blocks in pieces:
        draws = jax.random.uniform(jax.random.fold_in(jax.random.fold_in(stream_key, 6), dim), (blocks,), jnp.float32, low / len(pieces), high / len(pieces))
        level = level * jnp.repeat(jnp.exp(draws), extent[dim] // blocks).reshape((-1,) + (1,) * (len(extent) - 1 - dim))
    return level


def bell_draw(stream_key, shape, scale, most, cuts=(), held_as=jnp.bfloat16):
    level = levels(stream_key, shape, cuts, -0.22, 0.18) if cuts else 1.0
    result = jax.random.normal(stream_key, shape, jnp.float32) * scale * level
    return jnp.minimum(jnp.maximum(result, -most), most).astype(held_as)


def setup_inputs(seed: int = 0) -> dict:
    streams_of = jax.random.split(jax.random.key(seed), 10)
    patches = bell_draw(streams_of[0], (N_DP, N_FSDP, TOK_MAX, PATCH), 1.0, 6.0, ((0, 8), (1, 4)))
    noise = bell_draw(streams_of[1], (N_DP, N_FSDP, TOK_MAX, PATCH), 1.0, 6.0, ((0, 8), (1, 4)))
    bucket = touch_ends(jax.random.randint(streams_of[2], (N_DP, N_FSDP), 0, BUCKETS), jax.random.fold_in(streams_of[2], 1), 0, BUCKETS - 1).astype(jnp.int32)
    tstep = touch_ends(jax.random.randint(streams_of[3], (N_DP, N_FSDP), 0, TSTEPS), jax.random.fold_in(streams_of[3], 1), 0, TSTEPS - 1).astype(jnp.int32)
    dest = draw_dest(jax.random.fold_in(streams_of[9], 71), 0)
    embed_weight = bell_draw(streams_of[5], (PATCH, D), PATCH ** -0.5, 0.75)
    gain = jnp.clip(1.0 + 0.18 * jax.random.normal(streams_of[6], (D,), jnp.float32), 0.1, 1.9)
    proj_weight = bell_draw(streams_of[7], (D, HW), D ** -0.5, 0.125, ((0, 4),))
    cotangent = bell_draw(streams_of[8], (N_DP, N_FSDP, CAP, TOK_MAX, HW), 1.0, 6.0, ((0, 8), (1, 4)))
    return dict(patches=patches, noise=noise, bucket=bucket, tstep=tstep, dest=dest, embed_weight=embed_weight, gain=gain, proj_weight=proj_weight, cotangent=cotangent)


norm_eps = 1e-06

def lengths_of(bucket):
    stride = max(1, TOK_MAX // (2 * BUCKETS))
    return (TOK_MAX - bucket * stride).astype(jnp.int32)

def noise_level(tstep, length):
    frac = (tstep.astype(jnp.float32) + 1.0) / TSTEPS
    shift = 1.0 + 2.0 * length.astype(jnp.float32) / TOK_MAX
    return shift * frac / (1.0 + (shift - 1.0) * frac)

def reference(patches, noise, bucket, tstep, dest, embed_weight, gain, proj_weight, cotangent):
    length = lengths_of(bucket)
    level = noise_level(tstep, length)[:, :, None, None]
    rows = jnp.arange(TOK_MAX, dtype=jnp.int32)
    mixed = (1.0 - level) * patches.astype(jnp.float32) + level * noise.astype(jnp.float32)
    latent = jnp.where(rows[None, None, :, None] < length[:, :, None, None], mixed, 0.0).astype(jnp.bfloat16)
    flat = latent.reshape(N_DP, N_FSDP, TOK_MAX * PATCH).astype(jnp.float32)
    ids = jnp.arange(N_DP, dtype=jnp.int32)
    same = dest[:, None, :] == dest[None, :, :]
    earlier = (ids[None, :] < ids[:, None])[:, :, None]
    slot = lax.optimization_barrier(jnp.sum((same & earlier).astype(jnp.int32), axis=1))
    slot_ids = jnp.arange(CAP, dtype=jnp.int32)
    width = proj_weight.shape[1]
    gain_float = gain.astype(jnp.float32)

    def owner_step(total, owner):
        pick = (dest[None, :, :] == owner) & (slot[None, :, :] == slot_ids[:, None, None])
        packed = jnp.einsum('cif,ifx->fcx', pick.astype(jnp.float32), flat).astype(jnp.bfloat16)
        packed = packed.reshape(N_FSDP * CAP * TOK_MAX, PATCH)
        plen = lax.optimization_barrier(jnp.sum(jnp.where(pick, length[None, :, :], 0), axis=1)).astype(jnp.int32)
        valid = rows[None, None, :] < plen.T[:, :, None]
        hidden = jnp.dot(packed, embed_weight, preferred_element_type=jnp.float32)
        centered_input = hidden - lax.optimization_barrier(jnp.mean(hidden, axis=1, keepdims=True))
        inverse_deviation = lax.rsqrt(lax.optimization_barrier(jnp.mean(centered_input * centered_input, axis=1, keepdims=True)) + norm_eps)
        standardized_input = centered_input * inverse_deviation
        normed_rows = (standardized_input * gain_float).astype(jnp.bfloat16)
        output = jnp.dot(normed_rows, proj_weight, preferred_element_type=jnp.float32).astype(jnp.bfloat16)
        cot = lax.dynamic_index_in_dim(cotangent, owner, 0, keepdims=False)
        masked = jnp.where(valid[:, :, :, None], cot, jnp.zeros_like(cot)).reshape(N_FSDP * CAP * TOK_MAX, width)
        back = jnp.dot(masked, proj_weight.T, preferred_element_type=jnp.float32)
        input_gradient = back * gain_float
        hidden_gradient = (input_gradient - lax.optimization_barrier(jnp.mean(input_gradient, axis=1, keepdims=True)) - standardized_input * lax.optimization_barrier(jnp.mean(input_gradient * standardized_input, axis=1, keepdims=True))) * inverse_deviation
        hidden_gradient = hidden_gradient.astype(jnp.bfloat16)
        partial_value = lax.dot_general(packed, hidden_gradient, (((0,), (0,)), ((), ())), preferred_element_type=jnp.float32)
        return (total + partial_value, output.reshape(N_FSDP, CAP, TOK_MAX, width))
    total, projected = lax.scan(owner_step, jnp.zeros((PATCH, embed_weight.shape[1]), jnp.float32), ids)
    embed_grad = total * float(N_DP * N_FSDP * TOK_MAX) ** (-0.5)
    return (projected, embed_grad)
```

```python
import functools

import jax
import jax.numpy as jnp
from jax import lax
from jax.experimental import pallas as pl
from jax.experimental.pallas import tpu as pltpu
from jax.sharding import PartitionSpec as P

BUCKETS = 12
TSTEPS = 1000
EPS = 1e-06
F32 = jnp.float32
BF16 = jnp.bfloat16
MESH = pl.DeviceIdType.MESH
NT = (((1,), (1,)), ((), ()))
PIECES = 4


def cut(rows, pieces):
    step = -(-rows // (16 * pieces)) * 16
    return [(a, min(step, rows - a)) for a in range(0, rows, step)]


def kernel(
    n_dp, n_fs, share, owners, quota,
    bucket, tstep, dest, patches, noise, embed, gain, weight, cot,
    out, grad,
    lat, arr, packed, packed_t, masked, full, emb, gains, xhat, normed, gs, acc, obuf, stats,
    st, ra, sb, rb, fd, ff,
    lat_s, lat_r, own_s, own_r, y_s, y_r, x_s, x_r, pa_s, pa_r, pb_s, pb_r,
    a_s, a_r, b_s, b_r, c_s, c_r, d_s, d_r, o_s,
):
    dp, fs = lax.axis_index("dp"), lax.axis_index("fsdp")
    y, c = fs // 2, fs % 2
    n_y = n_fs // 2
    cap, tok, width = cot.shape
    feats = patches.shape[1]
    dim = embed.shape[1]
    depth = weight.shape[0]
    unit = depth // share
    units = n_fs * share
    half = tok // 2
    h = dp % 2 if share == 2 else 0
    mate = dp + 1 - 2 * (dp % 2)
    partner = y * 2 + 1 - c

    def shard(j, core):
        return ((y + j) % n_y) * 2 + core

    def copy(src, dst, send, recv, to):
        return pltpu.make_async_remote_copy(
            src_ref=src, dst_ref=dst, send_sem=send, recv_sem=recv,
            device_id={"dp": to[0], "fsdp": to[1]}, device_id_type=MESH,
        )

    barrier = pltpu.get_barrier_semaphore()
    for k in range(1, n_dp):
        pl.semaphore_signal(
            barrier, inc=1, device_id={"dp": (dp + k) % n_dp, "fsdp": fs}, device_id_type=MESH
        )
    for k in range(1, n_fs):
        pl.semaphore_signal(
            barrier, inc=1, device_id={"dp": dp, "fsdp": (fs + k) % n_fs}, device_id_type=MESH
        )

    stride = max(1, tok // (2 * BUCKETS))
    my_len = tok - stride * bucket[dp, 0]
    frac = (jnp.full((1, feats), tstep[0, 0]).astype(F32) + 1.0) / TSTEPS
    shift = 1.0 + 2.0 * jnp.full((1, feats), my_len).astype(F32) / tok
    level = shift * frac / (1.0 + (shift - 1.0) * frac)
    rows = lax.broadcasted_iota(jnp.int32, (tok, feats), 0)
    mixed = (1.0 - level) * patches[...].astype(F32) + level * noise[...].astype(F32)
    mixed = jnp.where(rows < my_len, mixed, 0.0)
    mine = jnp.concatenate([mixed[:half], mixed[half:]], axis=1).astype(BF16)
    lat[...] = mine
    arr[dp] = mine

    pl.semaphore_wait(barrier, n_dp + n_fs - 2)

    sends = []
    lats = []
    for k in range(1, n_dp):
        cp = copy(lat, arr.at[dp], lat_s.at[k], lat_r.at[k], ((dp + k) % n_dp, fs))
        cp.start()
        lats.append(cp)
    parts = cut(unit, PIECES)
    base = pl.multiple_of(h * unit, 16) if share == 2 else 0
    other = pl.multiple_of((1 - h) * unit, 16) if share == 2 else 0
    ys = {}
    for j in range(1, n_y):
        for p, (at, size) in enumerate(parts):
            sel = pl.ds(pl.multiple_of(base + at, 16), size)
            ys[j, p] = copy(
                weight.at[sel], full.at[fs, sel], y_s.at[j, p], y_r.at[j, p],
                (dp, ((y + n_y - j) % n_y) * 2 + c),
            )
            ys[j, p].start()
    own = copy(weight, full.at[fs], own_s, own_r, (dp, partner))
    own.start()

    count = jnp.int32(0)
    plen = [jnp.int32(0)] * cap
    chosen = []
    for i in range(n_dp):
        hit = (dest[i, 0] == dp).astype(jnp.int32)
        pick = [hit * (count == s).astype(jnp.int32) for s in range(cap)]
        length = tok - stride * bucket[i, 0]
        plen = [a + b * length for a, b in zip(plen, pick)]
        chosen.append(pick)
        count = count + hit
    cot_rows = lax.broadcasted_iota(jnp.int32, (tok, width), 0)
    for s in range(cap):
        masked[s * tok : (s + 1) * tok] = jnp.where(
            cot_rows < plen[s], cot[s].astype(F32), 0.0
        ).astype(BF16)
    for u in range(units):
        emb[u] = embed[:, u * unit : (u + 1) * unit]
        gains[u] = gain[:, u * unit : (u + 1) * unit]

    def block(w_ref, row):
        return w_ref[pl.ds(pl.multiple_of(row, 8), unit), :]

    def back(u, w):
        got = lax.dot_general(masked[...], w, NT, preferred_element_type=F32)
        gs[u] = got * gains[u]

    def sums(u):
        g = gs[u]
        stats[2] += jnp.sum(g, axis=1, keepdims=True)
        stats[3] += jnp.sum(g * xhat[u], axis=1, keepdims=True)

    def project(u, w):
        acc[...] += jnp.dot(normed[u], w, preferred_element_type=F32)

    @pl.loop(0, share)
    def _(i):
        back(fs * share + i, block(weight, i * unit))

    acc[...] = jnp.zeros_like(acc)
    stats[...] = jnp.zeros_like(stats)

    for cp in lats:
        cp.wait_recv()
    for s in range(cap):
        total = jnp.zeros((half, 2 * feats), F32)
        for i in range(n_dp):
            total += jnp.where(chosen[i][s] > 0, arr[i].astype(F32), 0.0)
        packed[s * tok : s * tok + half] = total[:, :feats].astype(BF16)
        packed[s * tok + half : (s + 1) * tok] = total[:, feats:].astype(BF16)
    packed_t[...] = packed[...].astype(F32).T.astype(BF16)

    @pl.loop(0, units)
    def _(u):
        hid = jnp.dot(packed[...], emb[u], preferred_element_type=F32)
        xhat[u] = hid
        stats[0] += jnp.sum(hid, axis=1, keepdims=True)

    mean = stats[0] * (1.0 / dim)

    @pl.loop(0, units)
    def _(u):
        cen = xhat[u] - mean
        xhat[u] = cen
        stats[1] += jnp.sum(cen * cen, axis=1, keepdims=True)

    rstd = lax.rsqrt(stats[1] * (1.0 / dim) + EPS)

    @pl.loop(0, units)
    def _(u):
        std = xhat[u] * rstd
        xhat[u] = std
        normed[u] = (std * gains[u]).astype(BF16)

    relayed = {}

    def relay_y(j, p):
        at, size = parts[p]
        ys[j, p].wait_recv()
        sel = pl.ds(pl.multiple_of(base + at, 16), size)
        src = full.at[shard(j, c), sel]
        if share == 2:
            cp = copy(src, src, x_s.at[j, p], x_r.at[j, p], (mate, fs))
            cp.start()
            relayed["x", j, p] = cp
        cp = copy(src, src, pa_s.at[j, p], pa_r.at[j, p], (dp, partner))
        cp.start()
        relayed["pa", j, p] = cp

    def relay_x(j, p):
        at, size = parts[p]
        relayed["x", j, p].wait_recv()
        sel = pl.ds(pl.multiple_of(other + at, 16), size)
        src = full.at[shard(j, c), sel]
        cp = copy(src, src, pb_s.at[j, p], pb_r.at[j, p], (dp, partner))
        cp.start()
        relayed["pb", j, p] = cp

    last = len(parts)
    firsts = [(1, p) for p in range(last)] if n_y > 1 else []
    for key in firsts[:1]:
        relay_y(*key)

    @pl.loop(0, share)
    def _(i):
        u = fs * share + i
        sums(u)
        project(u, block(weight, i * unit))

    for key in firsts[1:2]:
        relay_y(*key)
    own.wait_recv()

    def work(s, part):
        u = s * share + part
        w = block(full.at[s], part * unit)
        back(u, w)
        sums(u)
        project(u, w)

    @pl.loop(0, share)
    def _(i):
        work(partner, i)

    for j in range(1, n_y):
        for p in range(last):
            if ("pa", j, p) not in relayed:
                relay_y(j, p)
        work(shard(j, c), h)
        if share == 2:
            for p in range(last // 2):
                relay_x(j, p)
        for p in range(last):
            relayed["pa", j, p].wait_recv()
        work(shard(j, 1 - c), h)
        if share == 2:
            for p in range(last // 2, last):
                relay_x(j, p)
            work(shard(j, c), 1 - h)
            for p in range(last):
                relayed["pb", j, p].wait_recv()
            work(shard(j, 1 - c), 1 - h)

    mean_g = stats[2] * (1.0 / dim)
    mean_gx = stats[3] * (1.0 / dim)
    span = share * feats

    @pl.loop(0, n_fs)
    def _(s):
        for i in range(share):
            u = s * share + i
            dh = ((gs[u] - mean_g - xhat[u] * mean_gx) * rstd).astype(BF16)
            st[s, i * feats : (i + 1) * feats] = jnp.dot(
                packed_t[...], dh, preferred_element_type=F32
            ).astype(BF16)

    phase = []
    for k in range(1, n_fs):
        to = (fs + k) % n_fs
        cp = copy(st.at[to], ra.at[k], a_s.at[k], a_r.at[k], (dp, to))
        cp.start()
        phase.append(cp)

    obuf[...] = acc[...].astype(BF16)
    write = pltpu.make_async_copy(obuf, out, o_s)
    write.start()

    total = st[fs].astype(F32)
    for k, cp in enumerate(phase):
        cp.wait_recv()
        total += ra[k + 1].astype(F32)
    sb[...] = total.astype(BF16)
    sends += phase

    everyone = owners == n_dp

    def guard(cond, action):
        if everyone:
            action()
        else:
            pl.when(cond)(action)

    def piece(d):
        return pl.ds(pl.multiple_of(d * quota, 16), quota)

    owner = dp < owners
    scatter, spread = {}, {}
    for k in range(1, n_dp):
        to = (dp + k) % n_dp
        safe = to if everyone else to % owners
        scatter[k] = copy(sb.at[piece(safe)], rb.at[k], b_s.at[k], b_r.at[k], (to, fs))
        guard(to < owners, scatter[k].start)

    here = piece(dp if everyone else dp % owners)

    def reduce():
        mine = sb[here].astype(F32)
        for k in range(1, n_dp):
            scatter[k].wait_recv()
            mine += rb[k].astype(F32)
        fd[here] = mine.astype(BF16)

    guard(owner, reduce)
    for k in range(1, n_dp):
        to = (dp + k) % n_dp
        spread[k] = copy(fd.at[here], fd.at[here], c_s.at[k], c_r.at[k], (to, fs))
        guard(owner, spread[k].start)
    for k in range(1, n_dp):
        source = (dp + n_dp - k) % n_dp
        guard(source < owners, spread[k].wait_recv)

    phase = []
    for k in range(1, n_fs):
        to = (fs + k) % n_fs
        cp = copy(fd, ff.at[fs], d_s.at[k], d_r.at[k], (dp, to))
        cp.start()
        phase.append(cp)
    ff[fs] = fd[...]
    for cp in phase:
        cp.wait_recv()
    sends += phase
    scale = float(n_dp * n_fs * tok) ** (-0.5)
    for u in range(units):
        s, i = u // share, u % share
        grad[:, u * unit : (u + 1) * unit] = (
            ff[s, i * feats : (i + 1) * feats].astype(F32) * scale
        )

    write.wait()
    for cp in lats + [own] + list(ys.values()) + list(relayed.values()) + sends:
        cp.wait_send()
    for k in range(1, n_dp):
        to = (dp + k) % n_dp
        guard(to < owners, scatter[k].wait_send)
        guard(owner, spread[k].wait_send)


def body(patches, noise, bucket, tstep, dest, embed_weight, gain, proj_weight, cotangent):
    n_dp = lax.axis_size("dp")
    n_fs = lax.axis_size("fsdp")
    tok, feats = patches.shape[2:]
    depth, width = proj_weight.shape
    dim = gain.shape[0]
    cap = cotangent.shape[2]
    share = 2 if n_dp % 2 == 0 and depth % 32 == 0 else 1
    unit = depth // share
    units = n_fs * share
    rows = cap * tok
    span = share * feats
    quota = -(-span // (16 * n_dp)) * 16
    owners = span // quota
    n_y = n_fs // 2
    pieces = len(cut(unit, PIECES))
    vmem = pl.BlockSpec(memory_space=pltpu.VMEM)
    smem = pl.BlockSpec(memory_space=pltpu.SMEM)
    dma = pltpu.SemaphoreType.DMA
    link = dma((n_y, pieces))
    projected, grad = pl.pallas_call(
        functools.partial(kernel, n_dp, n_fs, share, owners, quota),
        out_shape=(
            jax.ShapeDtypeStruct((rows, width), BF16),
            jax.ShapeDtypeStruct((feats, dim), F32),
        ),
        in_specs=[smem] * 3 + [vmem] * 6,
        out_specs=(pl.BlockSpec(memory_space=pl.ANY), vmem),
        scratch_shapes=[
            pltpu.VMEM((tok // 2, 2 * feats), BF16),
            pltpu.VMEM((n_dp, tok // 2, 2 * feats), BF16),
            pltpu.VMEM((rows, feats), BF16),
            pltpu.VMEM((feats, rows), BF16),
            pltpu.VMEM((rows, width), BF16),
            pltpu.VMEM((n_fs, depth, width), BF16),
            pltpu.VMEM((units, feats, unit), BF16),
            pltpu.VMEM((units, 1, unit), F32),
            pltpu.VMEM((units, rows, unit), F32),
            pltpu.VMEM((units, rows, unit), BF16),
            pltpu.VMEM((units, rows, unit), F32),
            pltpu.VMEM((rows, width), F32),
            pltpu.VMEM((rows, width), BF16),
            pltpu.VMEM((4, rows, 1), F32),
            pltpu.VMEM((n_fs, span, unit), BF16),
            pltpu.VMEM((n_fs, span, unit), BF16),
            pltpu.VMEM((span, unit), BF16),
            pltpu.VMEM((n_dp, quota, unit), BF16),
            pltpu.VMEM((span, unit), BF16),
            pltpu.VMEM((n_fs, span, unit), BF16),
            dma((n_dp,)), dma((n_dp,)), dma, dma,
            link, link, link, link, link, link, link, link,
            dma((n_fs,)), dma((n_fs,)), dma((n_dp,)), dma((n_dp,)),
            dma((n_dp,)), dma((n_dp,)), dma((n_fs,)), dma((n_fs,)), dma,
        ],
        compiler_params=pltpu.CompilerParams(
            collective_id=0, has_side_effects=True, vmem_limit_bytes=62 * 1024 * 1024
        ),
    )(
        bucket, tstep, dest, patches[0, 0], noise[0, 0], embed_weight, gain[None],
        proj_weight, cotangent[0, 0],
    )
    return projected.reshape(1, 1, cap, tok, width), grad


def solution(mesh):
    placed = (
        P("dp", "fsdp", None, None),
        P("dp", "fsdp", None, None),
        P(None, "fsdp"),
        P("dp", "fsdp"),
        P(None, "fsdp"),
        P(),
        P(),
        P("fsdp", None),
        P("dp", "fsdp", None, None, None),
    )
    return jax.shard_map(
        body,
        mesh=mesh,
        in_specs=placed,
        out_specs=(P("dp", "fsdp", None, None, None), P()),
        check_vma=False,
    )
```

```python
import functools

import jax
import jax.numpy as jnp
from jax import lax
from jax.experimental import pallas as pl
from jax.experimental.pallas import tpu as pltpu
from jax.sharding import PartitionSpec as P

BUCKETS = 12
TSTEPS = 1000
EPS = 1e-06
F32 = jnp.float32
BF16 = jnp.bfloat16
MESH = pl.DeviceIdType.MESH
NT = (((1,), (1,)), ((), ()))
PIECES = 4


def cut(rows, pieces):
    step = -(-rows // (16 * pieces)) * 16
    return [(a, min(step, rows - a)) for a in range(0, rows, step)]


def kernel(
    n_dp, n_fs, share, owners, quota,
    bucket, tstep, dest, patches, noise, embed, gain, weight, cot,
    out, grad,
    lat, arr, packed, packed_t, masked, full, emb, gains, xhat, normed, gs, acc, stats,
    st, ra, sb, rb, fd, ff,
    lat_s, lat_r, own_s, own_r, y_s, y_r, x_s, x_r, pa_s, pa_r, pb_s, pb_r,
    a_s, a_r, b_s, b_r, c_s, c_r, d_s, d_r,
):
    dp, fs = lax.axis_index("dp"), lax.axis_index("fsdp")
    y, c = fs // 2, fs % 2
    n_y = n_fs // 2
    cap, tok, width = cot.shape
    feats = patches.shape[0]
    dim = embed.shape[1]
    depth = weight.shape[0]
    unit = depth // share
    units = n_fs * share
    half = tok // 2
    h = dp % 2 if share == 2 else 0
    mate = dp + 1 - 2 * (dp % 2)
    partner = y * 2 + 1 - c

    def shard(j, core):
        return ((y + j) % n_y) * 2 + core

    def copy(src, dst, send, recv, to):
        return pltpu.make_async_remote_copy(
            src_ref=src, dst_ref=dst, send_sem=send, recv_sem=recv,
            device_id={"dp": to[0], "fsdp": to[1]}, device_id_type=MESH,
        )

    barrier = pltpu.get_barrier_semaphore()
    for k in range(1, n_dp):
        pl.semaphore_signal(
            barrier, inc=1, device_id={"dp": (dp + k) % n_dp, "fsdp": fs}, device_id_type=MESH
        )
    for k in range(1, n_fs):
        pl.semaphore_signal(
            barrier, inc=1, device_id={"dp": dp, "fsdp": (fs + k) % n_fs}, device_id_type=MESH
        )

    stride = max(1, tok // (2 * BUCKETS))
    my_len = tok - stride * bucket[0, dp]
    frac = (jnp.full((1, tok), tstep[0, 0]).astype(F32) + 1.0) / TSTEPS
    shift = 1.0 + 2.0 * jnp.full((1, tok), my_len).astype(F32) / tok
    level = shift * frac / (1.0 + (shift - 1.0) * frac)
    rows = lax.broadcasted_iota(jnp.int32, (feats, tok), 1)
    mixed = (1.0 - level) * patches[...].astype(F32) + level * noise[...].astype(F32)
    mixed = jnp.where(rows < my_len, mixed, 0.0).T
    mine = jnp.concatenate([mixed[:half], mixed[half:]], axis=1).astype(BF16)
    lat[...] = mine
    arr[dp] = mine

    pl.semaphore_wait(barrier, n_dp + n_fs - 2)

    sends = []
    lats = []
    for k in range(1, n_dp):
        cp = copy(lat, arr.at[dp], lat_s.at[k], lat_r.at[k], ((dp + k) % n_dp, fs))
        cp.start()
        lats.append(cp)
    parts = cut(unit, PIECES)
    base = pl.multiple_of(h * unit, 16) if share == 2 else 0
    other = pl.multiple_of((1 - h) * unit, 16) if share == 2 else 0
    ys = {}
    for j in range(1, n_y):
        for p, (at, size) in enumerate(parts):
            sel = pl.ds(pl.multiple_of(base + at, 16), size)
            ys[j, p] = copy(
                weight.at[sel], full.at[fs, sel], y_s.at[j, p], y_r.at[j, p],
                (dp, ((y + n_y - j) % n_y) * 2 + c),
            )
            ys[j, p].start()
    own = copy(weight, full.at[fs], own_s, own_r, (dp, partner))
    own.start()

    count = jnp.int32(0)
    plen = [jnp.int32(0)] * cap
    chosen = []
    for i in range(n_dp):
        hit = (dest[0, i] == dp).astype(jnp.int32)
        pick = [hit * (count == s).astype(jnp.int32) for s in range(cap)]
        length = tok - stride * bucket[0, i]
        plen = [a + b * length for a, b in zip(plen, pick)]
        chosen.append(pick)
        count = count + hit
    cot_rows = lax.broadcasted_iota(jnp.int32, (tok, width), 0)
    for s in range(cap):
        masked[s * tok : (s + 1) * tok] = jnp.where(
            cot_rows < plen[s], cot[s].astype(F32), 0.0
        ).astype(BF16)
    line = jnp.concatenate([gain[t : t + 1] for t in range(gain.shape[0])], axis=1)
    for u in range(units):
        emb[u] = embed[:, u * unit : (u + 1) * unit]
        gains[u] = line[:, u * unit : (u + 1) * unit]

    def block(w_ref, row):
        return w_ref[pl.ds(pl.multiple_of(row, 8), unit), :]

    def back(u, w):
        got = lax.dot_general(masked[...], w, NT, preferred_element_type=F32)
        gs[u] = got * gains[u]

    def sums(u):
        g = gs[u]
        stats[2] += jnp.sum(g, axis=1, keepdims=True)
        stats[3] += jnp.sum(g * xhat[u], axis=1, keepdims=True)

    def project(u, w):
        acc[...] += jnp.dot(normed[u], w, preferred_element_type=F32)

    @pl.loop(0, share)
    def _(i):
        back(fs * share + i, block(weight, i * unit))

    acc[...] = jnp.zeros_like(acc)
    stats[...] = jnp.zeros_like(stats)

    for cp in lats:
        cp.wait_recv()
    for s in range(cap):
        total = jnp.zeros((half, 2 * feats), F32)
        for i in range(n_dp):
            total += jnp.where(chosen[i][s] > 0, arr[i].astype(F32), 0.0)
        packed[s * tok : s * tok + half] = total[:, :feats].astype(BF16)
        packed[s * tok + half : (s + 1) * tok] = total[:, feats:].astype(BF16)
    packed_t[...] = packed[...].astype(F32).T.astype(BF16)

    @pl.loop(0, units)
    def _(u):
        hid = jnp.dot(packed[...], emb[u], preferred_element_type=F32)
        xhat[u] = hid
        stats[0] += jnp.sum(hid, axis=1, keepdims=True)

    mean = stats[0] * (1.0 / dim)

    @pl.loop(0, units)
    def _(u):
        cen = xhat[u] - mean
        xhat[u] = cen
        stats[1] += jnp.sum(cen * cen, axis=1, keepdims=True)

    rstd = lax.rsqrt(stats[1] * (1.0 / dim) + EPS)

    @pl.loop(0, units)
    def _(u):
        std = xhat[u] * rstd
        xhat[u] = std
        normed[u] = (std * gains[u]).astype(BF16)

    relayed = {}

    def relay_y(j, p):
        at, size = parts[p]
        ys[j, p].wait_recv()
        sel = pl.ds(pl.multiple_of(base + at, 16), size)
        src = full.at[shard(j, c), sel]
        if share == 2:
            cp = copy(src, src, x_s.at[j, p], x_r.at[j, p], (mate, fs))
            cp.start()
            relayed["x", j, p] = cp
        cp = copy(src, src, pa_s.at[j, p], pa_r.at[j, p], (dp, partner))
        cp.start()
        relayed["pa", j, p] = cp

    def relay_x(j, p):
        at, size = parts[p]
        relayed["x", j, p].wait_recv()
        sel = pl.ds(pl.multiple_of(other + at, 16), size)
        src = full.at[shard(j, c), sel]
        cp = copy(src, src, pb_s.at[j, p], pb_r.at[j, p], (dp, partner))
        cp.start()
        relayed["pb", j, p] = cp

    last = len(parts)
    firsts = [(1, p) for p in range(last)] if n_y > 1 else []
    for key in firsts[:1]:
        relay_y(*key)

    @pl.loop(0, share)
    def _(i):
        u = fs * share + i
        sums(u)
        project(u, block(weight, i * unit))

    for key in firsts[1:2]:
        relay_y(*key)
    own.wait_recv()

    def work(s, part):
        u = s * share + part
        w = block(full.at[s], part * unit)
        back(u, w)
        sums(u)
        project(u, w)

    @pl.loop(0, share)
    def _(i):
        work(partner, i)

    for j in range(1, n_y):
        for p in range(last):
            if ("pa", j, p) not in relayed:
                relay_y(j, p)
        work(shard(j, c), h)
        if share == 2:
            for p in range(last // 2):
                relay_x(j, p)
        for p in range(last):
            relayed["pa", j, p].wait_recv()
        work(shard(j, 1 - c), h)
        if share == 2:
            for p in range(last // 2, last):
                relay_x(j, p)
            work(shard(j, c), 1 - h)
            for p in range(last):
                relayed["pb", j, p].wait_recv()
            work(shard(j, 1 - c), 1 - h)

    mean_g = stats[2] * (1.0 / dim)
    mean_gx = stats[3] * (1.0 / dim)
    span = share * feats

    def term(s):
        for i in range(share):
            u = s * share + i
            dh = ((gs[u] - mean_g - xhat[u] * mean_gx) * rstd).astype(BF16)
            st[s, i * feats : (i + 1) * feats] = jnp.dot(
                packed_t[...], dh, preferred_element_type=F32
            ).astype(BF16)

    phase = []
    for k in range(1, n_fs):
        to = (fs + k) % n_fs
        term(to)
        cp = copy(st.at[to], ra.at[k], a_s.at[k], a_r.at[k], (dp, to))
        cp.start()
        phase.append(cp)

    term(fs)
    out[...] = acc[...].astype(BF16)

    total = st[fs].astype(F32)
    for k, cp in enumerate(phase):
        cp.wait_recv()
        total += ra[k + 1].astype(F32)
    sb[...] = total.astype(BF16)
    sends += phase

    everyone = owners == n_dp

    def guard(cond, action):
        if everyone:
            action()
        else:
            pl.when(cond)(action)

    def piece(d):
        return pl.ds(pl.multiple_of(d * quota, 16), quota)

    owner = dp < owners
    scatter, spread = {}, {}
    for k in range(1, n_dp):
        to = (dp + k) % n_dp
        safe = to if everyone else to % owners
        scatter[k] = copy(sb.at[piece(safe)], rb.at[k], b_s.at[k], b_r.at[k], (to, fs))
        guard(to < owners, scatter[k].start)

    here = piece(dp if everyone else dp % owners)

    def reduce():
        mine = sb[here].astype(F32)
        for k in range(1, n_dp):
            scatter[k].wait_recv()
            mine += rb[k].astype(F32)
        fd[here] = mine.astype(BF16)

    guard(owner, reduce)
    for k in range(1, n_dp):
        to = (dp + k) % n_dp
        spread[k] = copy(fd.at[here], fd.at[here], c_s.at[k], c_r.at[k], (to, fs))
        guard(owner, spread[k].start)
    for k in range(1, n_dp):
        source = (dp + n_dp - k) % n_dp
        guard(source < owners, spread[k].wait_recv)

    phase = []
    for k in range(1, n_fs):
        to = (fs + k) % n_fs
        cp = copy(fd, ff.at[fs], d_s.at[k], d_r.at[k], (dp, to))
        cp.start()
        phase.append(cp)
    ff[fs] = fd[...]
    for cp in phase:
        cp.wait_recv()
    sends += phase
    scale = float(n_dp * n_fs * tok) ** (-0.5)
    for u in range(units):
        s, i = u // share, u % share
        grad[:, u * unit : (u + 1) * unit] = (
            ff[s, i * feats : (i + 1) * feats].astype(F32) * scale
        )

    for cp in lats + [own] + list(ys.values()) + list(relayed.values()) + sends:
        cp.wait_send()
    for k in range(1, n_dp):
        to = (dp + k) % n_dp
        guard(to < owners, scatter[k].wait_send)
        guard(owner, spread[k].wait_send)


def body(patches, noise, bucket, tstep, dest, embed_weight, gain, proj_weight, cotangent):
    n_dp = lax.axis_size("dp")
    n_fs = lax.axis_size("fsdp")
    tok, feats = patches.shape[2:]
    depth, width = proj_weight.shape
    dim = gain.shape[0]
    cap = cotangent.shape[2]
    share = 2 if n_dp % 2 == 0 and depth % 32 == 0 else 1
    unit = depth // share
    units = n_fs * share
    rows = cap * tok
    span = share * feats
    quota = -(-span // (16 * n_dp)) * 16
    owners = span // quota
    n_y = n_fs // 2
    pieces = len(cut(unit, PIECES))
    vmem = pl.BlockSpec(memory_space=pltpu.VMEM)
    smem = pl.BlockSpec(memory_space=pltpu.SMEM)
    dma = pltpu.SemaphoreType.DMA
    link = dma((n_y, pieces))
    projected, grad = pl.pallas_call(
        functools.partial(kernel, n_dp, n_fs, share, owners, quota),
        out_shape=(
            pltpu.VMEM((rows, width), BF16),
            pltpu.VMEM((feats, dim), F32),
        ),
        in_specs=[smem] * 3 + [vmem] * 6,
        out_specs=(vmem, vmem),
        scratch_shapes=[
            pltpu.VMEM((tok // 2, 2 * feats), BF16),
            pltpu.VMEM((n_dp, tok // 2, 2 * feats), BF16),
            pltpu.VMEM((rows, feats), BF16),
            pltpu.VMEM((feats, rows), BF16),
            pltpu.VMEM((rows, width), BF16),
            pltpu.VMEM((n_fs, depth, width), BF16),
            pltpu.VMEM((units, feats, unit), BF16),
            pltpu.VMEM((units, 1, unit), F32),
            pltpu.VMEM((units, rows, unit), F32),
            pltpu.VMEM((units, rows, unit), BF16),
            pltpu.VMEM((units, rows, unit), F32),
            pltpu.VMEM((rows, width), F32),
            pltpu.VMEM((4, rows, 1), F32),
            pltpu.VMEM((n_fs, span, unit), BF16),
            pltpu.VMEM((n_fs, span, unit), BF16),
            pltpu.VMEM((span, unit), BF16),
            pltpu.VMEM((n_dp, quota, unit), BF16),
            pltpu.VMEM((span, unit), BF16),
            pltpu.VMEM((n_fs, span, unit), BF16),
            dma((n_dp,)), dma((n_dp,)), dma, dma,
            link, link, link, link, link, link, link, link,
            dma((n_fs,)), dma((n_fs,)), dma((n_dp,)), dma((n_dp,)),
            dma((n_dp,)), dma((n_dp,)), dma((n_fs,)), dma((n_fs,)),
        ],
        compiler_params=pltpu.CompilerParams(
            collective_id=0, has_side_effects=True, vmem_limit_bytes=44 * 1024 * 1024
        ),
    )(
        bucket.T, tstep, dest.T, patches[0, 0].T, noise[0, 0].T, embed_weight,
        gain.reshape(-1, 128),
        proj_weight, cotangent[0, 0],
    )
    return projected.reshape(1, 1, cap, tok, width), grad


def solution(mesh):
    placed = (
        P("dp", "fsdp", None, None),
        P("dp", "fsdp", None, None),
        P(None, "fsdp"),
        P("dp", "fsdp"),
        P(None, "fsdp"),
        P(),
        P(),
        P("fsdp", None),
        P("dp", "fsdp", None, None, None),
    )
    return jax.shard_map(
        body,
        mesh=mesh,
        in_specs=placed,
        out_specs=(P("dp", "fsdp", None, None, None), P()),
        check_vma=False,
    )
```
